32 devices in a mesh: site: 2 (over y), pts: 4 (over z), var: 2 (over x), cmp: 2 (over core).
Axes of the slice: x: 2, y: 2, z: 4, core: 2. Of those that a mesh axis runs over, the one named last changes fastest.
Arguments:
- sgt: bfloat16 [6, 3, 128, 4096], P('cmp', None, ('site', 'pts')), parts along dimension 2, may hold values from -6 to 6
- moment: float32 [6, 64], P('cmp', ('site', 'pts')), parts along dimension 1, may hold values from -6 to 6
- slip_spec: float32 [16, 2, 4096], replicated, may hold values from -3 to 3
- rp_slab: int32 [64], P('site'), parts along dimension 0, may hold values from 0 to 63, as said below
- rup_counts: int32 [8, 6], P(('site', 'pts')), parts along dimension 0, may hold values from 1 to 2, 8 in all within a row
- var_rupture: int32 [32], P('site'), parts along dimension 0, may hold values from 0 to 5
- var_source: int32 [32, 2], P('site'), parts along dimension 0, may hold values from 0 to 15
- owner_map: int32 [32], P('site'), parts along dimension 0, may hold values from 0 to 15, each once
Outputs:
- seismograms: float32 [32, 3, 4096], P(('site', 'pts', 'var', 'cmp')), parts along dimension 0
The draws below stay inside these ranges and needn't reach their ends.
There are 2 independent parts, one for each index of `site`. The reference program is written for one: setup_inputs(seed, part) draws one part's arguments, and reference() takes and returns one part's arrays. A program takes and returns all parts, laid end to end along the dimension named above; an argument that names none is the same for every part. Nothing has to cross between parts.
Inputs may be any that keep to these rules, and one draw needn't show every extreme that they name: `rp_slab`: in each aligned block of 8 rupture-points (one owner's), at most 4 name slab points of one reader (slab points k * 16 to (k + 1) * 16 - 1 belong to reader k), and in every block some reader is named exactly 4 times. `rup_counts`: each row gives, for the ruptures in order, how many of that owner's 8 slots belong to each; every rupture has 1 or more on every owner, the row sums to 8, and some entry of each row is exactly 2. `owner_map`: A permutation of the variations.
All inputs are finite; a program needn't handle non-finite values.
Results may differ from the reference program's by a relative error of at most 0.0003.
Values may be sent and summed in bfloat16 or wider, within the bound.
A program may use at most 64 MiB of HBM per device.

```python
import math
import jax
import jax.numpy as jnp
import numpy as np
from jax import lax

NT = 4096
NMT = 6
NC = 3
TAU = 4
NSF = 16
NRUP = 6
RP_DEV = 8
SLAB_DEV = 16
MOSTP = 2
CAP = 4
OWNERS = 4
NRP = 32
NSLAB = 64
NVAR = 16


def draw_rp_slab(key, part):
    blocks = NRP // RP_DEV
    readers = NSLAB // SLAB_DEV
    pool_size = readers * CAP

    def one_block(block_key):
        key_first, key_scores, key_order, key_within = jax.random.split(block_key, 4)
        reader_of = jnp.arange(pool_size, dtype=jnp.int32) % readers
        first_reader = jax.random.randint(key_first, (), 0, readers, dtype=jnp.int32)
        scores = jax.random.randint(key_scores, (pool_size,), 0, 1 << 20, dtype=jnp.int32)
        scores = jnp.where(reader_of == first_reader, -1, scores)
        scores = scores * pool_size + jnp.arange(pool_size, dtype=jnp.int32)
        ordering = jnp.argsort(scores)
        chosen = reader_of[ordering][:RP_DEV]
        chosen = jax.random.permutation(key_order, chosen)
        within = jax.random.randint(key_within, (RP_DEV,), 0, SLAB_DEV, dtype=jnp.int32)
        return (chosen * SLAB_DEV + within).astype(jnp.int32)
    block_keys = jax.random.split(jax.random.fold_in(key, 17), blocks)
    return jax.vmap(one_block)(block_keys).reshape(NRP)


def touch_ends(entries, stream_key, smallest, top_value):
    index_at = [jax.random.randint(jax.random.fold_in(stream_key, axis), (), 0, length) for axis, length in enumerate(entries.shape)]
    longest = entries.shape.index(max(entries.shape))
    next_to = index_at[:longest] + [(index_at[longest] + 1) % entries.shape[longest]] + index_at[longest + 1:]
    return entries.at[tuple(index_at)].set(smallest).at[tuple(next_to)].set(top_value)


def level_of(key, shape, cuts, smallest, largest):
    def one(dim, blocks):
        draws = jax.random.uniform(jax.random.fold_in(jax.random.fold_in(key, 6), dim), (blocks,), jnp.float32, smallest / len(cuts), largest / len(cuts))
        return jnp.repeat(jnp.exp(draws), shape[dim] // blocks).reshape((-1,) + (1,) * (len(shape) - dim - 1))

    gain = one(*cuts[0])
    for cut in cuts[1:]:
        gain = gain * one(*cut)
    return gain


def rank_table(count, skew):
    weights = [(1 << 20) // math.isqrt(grade ** skew) + 1 for grade in range(1, count + 1)]
    scale = 1 + sum(weights) // (1 << 30)
    return np.cumsum(np.array([max(1, weight // scale) for weight in weights]))


def ranked(stream_key, dims, amount, slope):
    listing = rank_table(amount, slope)
    pick = jax.random.randint(jax.random.fold_in(stream_key, 1), dims, 0, int(listing[amount - 1]))
    rank = jnp.searchsorted(jnp.asarray(listing, jnp.int32), pick, side="right")
    return jax.random.permutation(jax.random.fold_in(stream_key, 2), amount)[rank].astype(jnp.int32)


def length_profile(number_of, total, bound, lean):
    loads = [(1 << 20) // math.isqrt(grade ** lean) + 1 for grade in range(2, number_of + 1)]
    rest, counts = total - bound - (number_of - 1), [1] * (number_of - 1)
    while rest > 0:
        movable = [i for i in range(number_of - 1) if counts[i] < bound]
        whole, left = sum([loads[i] for i in movable]), rest
        for i in movable:
            extra = min(bound - counts[i], max(1, left * loads[i] // whole), rest)
            counts[i] = counts[i] + extra
            rest = rest - extra
    return np.array([bound] + counts)


def ragged(stream_key, number_of, total, bound, slope):
    if number_of == 2:
        one = jax.random.randint(stream_key, (), max(1, total - bound), min(bound, total - 1) + 1)
        return jnp.stack([one, total - one])
    sizes = jnp.asarray(length_profile(number_of, total, bound, slope), jnp.int32)
    couples = (number_of - 1) // 2
    source_of, taker = sizes[1:1 + 2 * couples:2], sizes[2:2 + 2 * couples:2]
    slack = jnp.minimum(source_of - 1, bound - taker)
    moved = jax.random.randint(jax.random.fold_in(stream_key, 1), (couples,), 0, 1 << 20) % (slack + 1)
    sizes = sizes.at[1:1 + 2 * couples:2].set(source_of - moved).at[2:2 + 2 * couples:2].set(taker + moved)
    return sizes[jax.random.permutation(jax.random.fold_in(stream_key, 2), number_of)]


def normal_values(rng, shape, deviation, limit, cuts=(), held_as=jnp.bfloat16):
    values = jax.random.normal(rng, shape, jnp.float32) * deviation
    if len(cuts) > 0:
        values = level_of(rng, shape, cuts, -0.22, 0.18) * values
    return jnp.clip(values, min=-limit, max=limit).astype(held_as)


def setup_inputs(seed: int = 0, part: int = 0) -> dict:
    arg_keys = jax.random.split(jax.random.key(seed), 9)
    own_keys = jax.random.split(jax.random.fold_in(arg_keys[8], part), 9)
    return {
        "sgt": normal_values(own_keys[0], (NMT, NC, NSLAB, NT), 1.0, 6.0, ((0, 2), (2, 4))),
        "moment": normal_values(own_keys[1], (NMT, NRP), 0.4, 6.0, ((0, 2), (1, 4)), jnp.float32),
        "slip_spec": normal_values(arg_keys[2], (NSF, 2, NT), 0.2, 3.0, (), jnp.float32),
        "rp_slab": draw_rp_slab(jax.random.fold_in(jax.random.fold_in(arg_keys[8], part), 71), part),
        "rup_counts": jax.vmap(lambda own: ragged(own, NRUP, RP_DEV, MOSTP, 2))(jax.random.split(own_keys[4], OWNERS)).reshape((OWNERS, NRUP)).astype(jnp.int32),
        "var_rupture": touch_ends(ranked(own_keys[5], (NVAR,), NRUP, 2), jax.random.fold_in(own_keys[5], 3), 0, NRUP - 1).astype(jnp.int32),
        "var_source": touch_ends(jax.random.randint(own_keys[6], (NVAR, 2), 0, NSF), jax.random.fold_in(own_keys[6], 1), 0, NSF - 1).astype(jnp.int32),
        "owner_map": jax.random.permutation(own_keys[7], NVAR).astype(jnp.int32),
    }


def reference(sgt, moment, slip_spec, rp_slab, rup_counts, var_rupture, var_source, owner_map):
    samples = sgt.shape[3]
    length = 2 * samples
    owners = rup_counts.shape[0]
    rp_dev = rp_slab.shape[0] // owners
    functions = slip_spec.shape[0]

    def owner_spectra(owner_index):
        start_row = (owner_index * rp_dev).astype(jnp.int32)
        slab_rows = lax.dynamic_slice_in_dim(rp_slab, start_row, rp_dev, 0)
        weights = lax.dynamic_slice_in_dim(moment, start_row, rp_dev, 1)
        picked = jnp.take(sgt, slab_rows, axis=2).astype(jnp.float32)
        signal = jnp.sum(weights[:, None, :, None] * picked, axis=0)
        return jnp.fft.rfft(signal, n=length, axis=-1)[..., :samples]

    spectra = lax.map(owner_spectra, jnp.arange(owners, dtype=jnp.int32))
    spectra = jnp.moveaxis(spectra, 1, 2).reshape(owners * rp_dev, 3, samples)

    slot_iota = jnp.arange(rp_dev, dtype=jnp.int32)
    inclusive = jnp.cumsum(rup_counts, axis=1).astype(jnp.int32)
    rupture_of = jnp.sum(inclusive[:, None, :] <= slot_iota[None, :, None], axis=2).astype(jnp.int32)
    before = (jnp.cumsum(rup_counts, axis=0) - rup_counts).astype(jnp.int32)
    start_here = (inclusive - rup_counts).astype(jnp.int32)
    position = slot_iota[None, :] - jnp.take_along_axis(start_here, rupture_of, 1) + jnp.take_along_axis(before, rupture_of, 1)
    rupture_flat = rupture_of.reshape(-1)
    position_flat = position.reshape(-1).astype(jnp.int32)
    lengths = jnp.sum(rup_counts, axis=0).astype(jnp.int32)
    frequency = jnp.arange(samples, dtype=jnp.int32)

    def one_slot(slot_index):
        variation = owner_map[slot_index]
        rupture = var_rupture[variation]
        hypocenter = (var_source[variation, 0] * lengths[rupture]) // functions
        delays = (TAU * jnp.abs(position_flat - hypocenter)).astype(jnp.int32)
        numerator = (delays[:, None] * frequency[None, :]) % length
        angles = numerator.astype(jnp.float32) * (2.0 * math.pi / length)
        members = (rupture_flat == rupture).astype(jnp.float32)
        phases = (jnp.cos(angles) - 1j * jnp.sin(angles)) * members[:, None]
        summed = jnp.einsum("qf,qcf->cf", phases, spectra, precision=lax.Precision.HIGHEST)
        slip_rows = slip_spec[var_source[variation, 1]]
        product_spec = summed * (slip_rows[0] + 1j * slip_rows[1])[None, :]
        padded = jnp.concatenate([jnp.real(product_spec[:, :1]) + 0.0 * product_spec[:, :1], product_spec[:, 1:], jnp.zeros_like(product_spec[:, :1])], axis=1)
        return jnp.fft.irfft(padded, n=length, axis=-1)[:, :samples].astype(jnp.float32)

    return lax.map(one_slot, jnp.arange(owner_map.shape[0], dtype=jnp.int32))
```

```python
import functools
import math

import jax
import jax.numpy as jnp
import numpy as np
from jax import lax
from jax.experimental import pallas as pl
from jax.experimental.pallas import tpu as pltpu
from jax.sharding import PartitionSpec as P

TAU = 4
MOST = 2
LANES = 128
MESH = pl.DeviceIdType.MESH
HIGHEST = lax.Precision.HIGHEST


def ceil_to(value, unit):
    return (value + unit - 1) // unit * unit


def tables(comps, samples, tail_rows, row_pitch):
    length = 2 * samples
    blocks = length // LANES
    half = blocks // 2
    outer = np.arange(blocks)

    def angle(numer, period):
        return 2.0 * np.pi * (numer % period) / period

    first = np.zeros((comps, 2 * blocks, row_pitch))
    for c in range(comps):
        for t1 in range(half + tail_rows):
            row = c * half + t1 if t1 < half else comps * half + (t1 - half) * comps + c
            turn = angle(outer * t1, blocks)
            first[c, :blocks, row] = np.cos(turn)
            first[c, blocks:, row] = -np.sin(turn)
    first = first.reshape(comps * 2 * blocks, row_pitch)
    lane = np.arange(LANES)
    turn = angle(outer[:, None] * lane[None, :], length)
    twiddle = np.stack([np.cos(turn), np.sin(turn)])
    group = lane // half
    k2 = 2 * (lane % half) + group // 2
    imag = group % 2
    turn = angle(lane[:, None] * k2[None, :], LANES)
    cos, sin = np.cos(turn), np.sin(turn)
    top = np.where(imag[None] == 1, -sin, cos)
    bottom = np.where(imag[None] == 1, cos, sin)
    top_swap = np.where(imag[None] == 0, -sin, cos)
    bottom_swap = np.where(imag[None] == 0, cos, sin)
    second = np.concatenate(
        [np.concatenate([top, top_swap], 1), np.concatenate([bottom, bottom_swap], 1)], 0
    )
    turn = angle(k2[:, None] * lane[None, :], LANES)
    cos, sin = np.cos(turn), np.sin(turn)
    third = np.concatenate(
        [np.where(imag[:, None] == 1, -sin, cos), np.where(imag[:, None] == 1, cos, sin)], 1
    )
    turn = angle(np.arange(half)[:, None] * outer[None, :], blocks)
    last = np.concatenate([np.cos(turn), -np.sin(turn)], 1)
    weight = np.full((blocks, LANES), 2.0 / length)
    weight[0, (lane % half == 0) & (group // 2 == 0)] = 1.0 / length
    return [np.asarray(t, np.float32) for t in (first, twiddle, second, third, last, weight)]


def dot(a, b, contract=(1, 0)):
    return lax.dot_general(
        a,
        b,
        (((contract[0],), (contract[1],)), ((), ())),
        precision=HIGHEST,
        preferred_element_type=jnp.float32,
    )


def kernel(
    dims,
    counts_ref,
    moment_ref,
    rupture_ref,
    source_ref,
    owner_ref,
    slab_ref,
    sgt_hbm,
    slip_hbm,
    first_hbm,
    twiddle_hbm,
    second_hbm,
    third_hbm,
    last_hbm,
    weight_hbm,
    out_ref,
    sgt_ref,
    slip_ref,
    first_ref,
    twiddle_ref,
    second_ref,
    third_ref,
    last_ref,
    weight_ref,
    meta_ref,
    slabs_ref,
    spect_ref,
    acc_ref,
    mine_ref,
    pair_ref,
    sums_ref,
    ring_ref,
    load_sem,
    meta_send,
    meta_recv,
    pair_send,
    pair_recv,
    ring_send,
    ring_recv,
):
    owners, variants, cores, lanes_q, delays, pitch, tail_rows = dims
    moments, comps, slab_dev, samples = sgt_ref.shape
    ruptures = counts_ref.shape[1]
    rp_dev = moment_ref.shape[1]
    nrp = slab_ref.shape[1]
    functions = slip_ref.shape[0]
    half = samples // LANES
    blocks = 2 * half
    nv = owners * cores
    me = lax.axis_index("pts")
    my_var = lax.axis_index("var")
    my_core = lax.axis_index("cmp")

    barrier = pltpu.get_barrier_semaphore()
    for d in range(1, owners):
        pl.semaphore_signal(
            barrier, inc=1, device_id={"pts": lax.rem(me + d, owners)}, device_id_type=MESH
        )
    for c in range(1, cores):
        pl.semaphore_signal(
            barrier, inc=1, device_id={"cmp": lax.rem(my_core + c, cores)}, device_id_type=MESH
        )
    loads = []
    for i, (src, dst) in enumerate(
        (
            (slip_hbm, slip_ref),
            (sgt_hbm, sgt_ref),
            (weight_hbm, weight_ref),
            (first_hbm, first_ref),
            (twiddle_hbm, twiddle_ref),
            (second_hbm, second_ref),
            (third_hbm, third_ref),
            (last_hbm, last_ref),
        )
    ):
        copy = pltpu.make_async_copy(src, dst, load_sem.at[i])
        copy.start()
        loads.append(copy)

    lane = lax.broadcasted_iota(jnp.int32, (1, lanes_q), 1)
    start = me * rp_dev
    slot = lane - start
    inside = (slot >= 0) & (slot < rp_dev)
    zero = jnp.zeros((1, lanes_q), jnp.float32)
    meta_ref[0] = jnp.zeros(meta_ref.shape[1:], jnp.float32)
    for j in range(moments):
        row = zero
        for l in range(rp_dev):
            row = jnp.where(slot == l, moment_ref[j, l], row)
        meta_ref[0, j : j + 1, :] = row
    total = jnp.int32(0)
    rup_row = jnp.zeros((1, lanes_q), jnp.int32)
    begin_row = jnp.zeros((1, lanes_q), jnp.int32)
    for r in range(ruptures):
        count = counts_ref[0, r]
        total = total + count
        passed = total <= slot
        rup_row = rup_row + passed.astype(jnp.int32)
        begin_row = jnp.where(passed, total, begin_row)
        value = count.astype(jnp.float32)
        meta_ref[0, 8 + r : 9 + r, :] = jnp.where(lane >= start + rp_dev, value, 0.0)
        meta_ref[0, 16 + r : 17 + r, :] = zero + value
    meta_ref[0, moments : moments + 1, :] = jnp.where(inside, rup_row.astype(jnp.float32), 0.0)
    meta_ref[0, moments + 1 : moments + 2, :] = jnp.where(
        inside, (slot - begin_row).astype(jnp.float32), 0.0
    )
    slabs_ref[...] = jnp.full(slabs_ref.shape, -1, jnp.int32)
    slabs_ref[:, :nrp] = slab_ref[...]

    rup_v = jnp.zeros((nv, lanes_q), jnp.float32)
    src_v = jnp.zeros((nv, lanes_q), jnp.float32)
    v_iota = lax.broadcasted_iota(jnp.int32, (nv, lanes_q), 0)
    my_slip = jnp.int32(0)
    for i in range(nv):
        p = lax.rem(me + i % owners, owners)
        c = lax.rem(my_core + i // owners, cores)
        var_id = owner_ref[(p * variants + my_var) * cores + c]
        rup_v = jnp.where(v_iota == i, rupture_ref[var_id].astype(jnp.float32), rup_v)
        src_v = jnp.where(v_iota == i, source_ref[var_id, 0].astype(jnp.float32), src_v)
        if i == 0:
            my_slip = source_ref[var_id, 1]

    pl.semaphore_wait(barrier, owners + cores - 2)
    metas = []
    for d in range(1, owners):
        copy = pltpu.make_async_remote_copy(
            src_ref=meta_ref.at[0],
            dst_ref=meta_ref.at[d],
            send_sem=meta_send.at[d],
            recv_sem=meta_recv.at[d],
            device_id={"pts": lax.rem(me + d, owners)},
            device_id_type=MESH,
        )
        copy.start()
        metas.append(copy)

    loads[0].wait()
    for a in range(half):
        real = slip_ref[my_slip, 0:1, a * LANES : (a + 1) * LANES]
        imag = slip_ref[my_slip, 1:2, a * LANES : (a + 1) * LANES]
        spect_ref[a : a + 1, :] = real
        spect_ref[half + a : half + a + 1, :] = real
        spect_ref[2 * half + a : 2 * half + a + 1, :] = -imag
        spect_ref[3 * half + a : 3 * half + a + 1, :] = imag
    turned = jnp.transpose(spect_ref[...])
    loads[2].wait()
    slip_real = weight_ref[...] * jnp.concatenate(
        [turned[:blocks, :blocks], turned[blocks:, :blocks]], axis=1
    )
    slip_imag = weight_ref[...] * jnp.concatenate(
        [turned[:blocks, blocks:], turned[blocks:, blocks:]], axis=1
    )
    spect_ref[:blocks, :] = slip_real
    spect_ref[blocks:, :] = slip_imag

    loads[1].wait()
    for copy in metas:
        copy.wait()
    merged = meta_ref[0]
    for d in range(1, owners):
        merged = merged + meta_ref[d]
    rup_row = merged[moments : moments + 1]
    pos_row = merged[moments + 1 : moments + 2]
    len_v = jnp.zeros((nv, lanes_q), jnp.float32)
    for r in range(ruptures):
        pos_row = pos_row + jnp.where(rup_row == r, merged[8 + r : 9 + r], 0.0)
        len_v = len_v + jnp.where(rup_v == r, merged[16 + r : 17 + r], 0.0)
    hyp_v = jnp.floor((src_v * len_v + 0.5) * (1.0 / functions))
    apart = jnp.where(rup_v == rup_row, jnp.abs(pos_row - hyp_v), -1.0)
    local = slabs_ref[...] - me * slab_dev
    s_iota = lax.broadcasted_iota(jnp.int32, (slab_dev, lanes_q), 0)
    hit = s_iota == local
    spread = jnp.concatenate(
        [jnp.where(hit, merged[j : j + 1], 0.0) for j in range(moments)] * 2, axis=0
    )
    depth = moments * slab_dev
    upper = lax.broadcasted_iota(jnp.int32, (1, 2 * depth), 1) < depth
    group = delays
    while group * nv > 64 and group % 2 == 0:
        group //= 2
    groups = delays // group
    width = samples + tail_rows * LANES
    if groups > 1:
        acc_ref[...] = jnp.zeros(acc_ref.shape, jnp.float32)

    def one_group(step, carry):
        base = (groups - 1 - step) * group
        picks = jnp.concatenate(
            [
                (apart == jnp.float32(delta) + lax.convert_element_type(base, jnp.float32)).astype(
                    jnp.float32
                )
                for delta in range(group)
            ],
            axis=0,
        )
        weights = dot(picks, spread, (1, 1))
        coarse = weights.astype(jnp.bfloat16)
        fine = (weights - coarse.astype(jnp.float32)).astype(jnp.bfloat16)
        pieces = jnp.where(upper, coarse.astype(jnp.float32), fine.astype(jnp.float32)).astype(
            jnp.bfloat16
        )
        pad = jnp.zeros((nv, width - samples), jnp.float32)
        for c in range(comps):
            series = jnp.concatenate([sgt_ref[j, c] for j in range(moments)] * 2, axis=0)
            product = jnp.dot(pieces, series, preferred_element_type=jnp.float32)
            acc = acc_ref[c] if groups > 1 else None
            for delta in reversed(range(group)):
                term = jnp.concatenate([product[delta * nv : (delta + 1) * nv], pad], axis=1)
                acc = term if acc is None else pltpu.roll(acc, TAU, 1) + term
            if groups > 1:
                acc_ref[c] = acc
            else:
                emit(c, acc)
        return carry

    def emit(c, acc):
        for t1 in range(half + tail_rows):
            row = c * half + t1 if t1 < half else comps * half + (t1 - half) * comps + c
            for b in range(nv // 8):
                mine_ref[pl.ds(b * 8 * pitch + row, 8, stride=pitch), :] = acc[
                    b * 8 : (b + 1) * 8, t1 * LANES : (t1 + 1) * LANES
                ]

    used = comps * (half + tail_rows)
    for i in range(nv):
        if used < pitch:
            mine_ref[i * pitch + used : (i + 1) * pitch, :] = jnp.zeros(
                (pitch - used, LANES), jnp.float32
            )
    if groups > 1:
        lax.fori_loop(0, groups, one_group, 0)
        for c in range(comps):
            emit(c, acc_ref[c])
    else:
        one_group(0, 0)

    size = owners * pitch
    pairs = []
    for c in range(1, cores):
        copy = pltpu.make_async_remote_copy(
            src_ref=mine_ref.at[pl.ds(c * size, size)],
            dst_ref=pair_ref.at[c - 1],
            send_sem=pair_send.at[c - 1],
            recv_sem=pair_recv.at[c - 1],
            device_id={"cmp": lax.rem(my_core + c, cores)},
            device_id_type=MESH,
        )
        copy.start()
        pairs.append(copy)
    for copy in loads[3:]:
        copy.wait()
    for copy in pairs:
        copy.wait_recv()
    order = sorted(range(1, owners), key=lambda d: -min(d, owners - d))

    def joined(d):
        value = mine_ref[d * pitch : (d + 1) * pitch, :]
        for c in range(1, cores):
            value = value + pair_ref[c - 1, d * pitch : (d + 1) * pitch, :]
        return value

    for d in order:
        sums_ref[d - 1] = joined(d)
    rings = []
    for d in order:
        copy = pltpu.make_async_remote_copy(
            src_ref=sums_ref.at[d - 1],
            dst_ref=ring_ref.at[d - 1],
            send_sem=ring_send.at[d - 1],
            recv_sem=ring_recv.at[d - 1],
            device_id={"pts": lax.rem(me + d, owners)},
            device_id_type=MESH,
        )
        copy.start()
        rings.append(copy)
    packed = joined(0)
    for copy in rings:
        copy.wait_recv()
    for d in range(1, owners):
        packed = packed + ring_ref[d - 1]

    stage = dot(first_ref[...], packed)
    cos, sin = twiddle_ref[0], twiddle_ref[1]
    rows = []
    for c in range(comps):
        real = stage[2 * c * blocks : (2 * c + 1) * blocks]
        imag = stage[(2 * c + 1) * blocks : (2 * c + 2) * blocks]
        rows.append(
            jnp.concatenate([real * cos + imag * sin, imag * cos - real * sin], axis=1)
        )
    spectra = dot(jnp.concatenate(rows, axis=0), second_ref[...])
    slip_real, slip_imag = spect_ref[:blocks, :], spect_ref[blocks:, :]
    rows = []
    for c in range(comps):
        part = spectra[c * blocks : (c + 1) * blocks]
        rows.append(part[:, :LANES] * slip_real + part[:, LANES:] * slip_imag)
    middle = dot(jnp.concatenate(rows, axis=0), third_ref[...])
    columns = []
    for c in range(comps):
        real = middle[c * blocks : (c + 1) * blocks, :LANES]
        imag = middle[c * blocks : (c + 1) * blocks, LANES:]
        columns.append(
            jnp.concatenate([real * cos - imag * sin, real * sin + imag * cos], axis=0)
        )
    result = dot(last_ref[...], jnp.concatenate(columns, axis=1))
    for c in range(comps):
        out_ref[c] = result[:, c * LANES : (c + 1) * LANES]
    for copy in pairs + rings:
        copy.wait_send()


def per_device(owners, variants, cores, *args):
    sgt, moment, slip_spec, rp_slab, rup_counts, var_rupture, var_source, owner_map = args
    moments, comps, slab_dev, samples = sgt.shape
    nrp = rp_slab.shape[0]
    half = samples // LANES
    nv = owners * cores
    assert owner_map.shape[0] == nv * variants and 4 * half == LANES and nv % 8 == 0
    assert moments + 2 <= 8 and rup_counts.shape[1] <= 8
    lanes_q = ceil_to(nrp, LANES)
    delays = MOST * owners
    tail_rows = ceil_to(TAU * (delays - 1), LANES) // LANES
    width = samples + tail_rows * LANES
    pitch = ceil_to(comps * (half + tail_rows), 8)
    consts = tables(comps, samples, tail_rows, pitch)
    dims = (owners, variants, cores, lanes_q, delays, pitch, tail_rows)
    f32 = jnp.float32
    others = max(owners - 1, 1)
    smem = pl.BlockSpec(memory_space=pltpu.SMEM)
    vmem = pl.BlockSpec(memory_space=pltpu.VMEM)
    anywhere = pl.BlockSpec(memory_space=pl.ANY)
    out = pl.pallas_call(
        functools.partial(kernel, dims),
        out_shape=jax.ShapeDtypeStruct((comps, half, LANES), f32),
        in_specs=[smem] * 5 + [vmem] + [anywhere] * 8,
        out_specs=vmem,
        scratch_shapes=[
            pltpu.VMEM(sgt.shape, sgt.dtype),
            pltpu.VMEM(slip_spec.shape, f32),
            *[pltpu.VMEM(t.shape, f32) for t in consts],
            pltpu.VMEM((owners, 24, lanes_q), f32),
            pltpu.VMEM((1, lanes_q), jnp.int32),
            pltpu.VMEM((LANES, LANES), f32),
            pltpu.VMEM((comps, nv, width) if nv * delays > 64 else (1, 8, LANES), f32),
            pltpu.VMEM((nv * pitch, LANES), f32),
            pltpu.VMEM((cores - 1, owners * pitch, LANES), f32),
            pltpu.VMEM((others, pitch, LANES), f32),
            pltpu.VMEM((others, pitch, LANES), f32),
            pltpu.SemaphoreType.DMA((8,)),
            pltpu.SemaphoreType.DMA((owners,)),
            pltpu.SemaphoreType.DMA((owners,)),
            pltpu.SemaphoreType.DMA((cores,)),
            pltpu.SemaphoreType.DMA((cores,)),
            pltpu.SemaphoreType.DMA((owners,)),
            pltpu.SemaphoreType.DMA((owners,)),
        ],
        compiler_params=pltpu.CompilerParams(collective_id=0, has_side_effects=True),
    )(
        rup_counts,
        moment,
        var_rupture,
        var_source,
        owner_map,
        rp_slab.reshape(1, nrp),
        sgt,
        slip_spec,
        *[jnp.asarray(t) for t in consts],
    )
    return out.reshape(1, comps, samples)


def solution(mesh):
    placed = (
        P("cmp", None, ("site", "pts"), None),
        P("cmp", ("site", "pts")),
        P(),
        P("site"),
        P(("site", "pts"), None),
        P("site"),
        P("site", None),
        P("site"),
    )
    sizes = (mesh.shape["pts"], mesh.shape["var"], mesh.shape["cmp"])
    return jax.shard_map(
        functools.partial(per_device, *sizes),
        mesh=mesh,
        in_specs=placed,
        out_specs=P(("site", "pts", "var", "cmp"), None, None),
        check_vma=False,
    )
```

```python
import functools
import math

import jax
import jax.numpy as jnp
import numpy as np
from jax import lax
from jax.experimental import pallas as pl
from jax.experimental.pallas import tpu as pltpu
from jax.sharding import PartitionSpec as P

TAU = 4
MOST = 2
LANES = 128
MESH = pl.DeviceIdType.MESH
HIGHEST = lax.Precision.HIGHEST


def ceil_to(value, unit):
    return (value + unit - 1) // unit * unit


def tables(comps, samples, tail_rows, tail_block):
    length = 2 * samples
    blocks = length // LANES
    half = blocks // 2
    outer = np.arange(blocks)

    def angle(numer, period):
        return 2.0 * np.pi * (numer % period) / period

    first = np.zeros((comps, 2 * blocks, tail_block + half))
    for c in range(comps):
        for t1 in range(half + tail_rows):
            row = tail_block + t1 if t1 < half else (t1 - half) * comps + c
            turn = angle(outer * t1, blocks)
            first[c, :blocks, row] = np.cos(turn)
            first[c, blocks:, row] = -np.sin(turn)
    lane = np.arange(LANES)
    turn = angle(outer[:, None] * lane[None, :], length)
    twiddle = np.stack([np.cos(turn), np.sin(turn)])
    group = lane // half
    k2 = 2 * (lane % half) + group // 2
    imag = group % 2
    turn = angle(lane[:, None] * k2[None, :], LANES)
    cos, sin = np.cos(turn), np.sin(turn)
    top = np.where(imag[None] == 1, -sin, cos)
    bottom = np.where(imag[None] == 1, cos, sin)
    top_swap = np.where(imag[None] == 0, -sin, cos)
    bottom_swap = np.where(imag[None] == 0, cos, sin)
    second = np.concatenate(
        [np.concatenate([top, top_swap], 1), np.concatenate([bottom, bottom_swap], 1)], 0
    )
    turn = angle(k2[:, None] * lane[None, :], LANES)
    cos, sin = np.cos(turn), np.sin(turn)
    third = np.concatenate(
        [np.where(imag[:, None] == 1, -sin, cos), np.where(imag[:, None] == 1, cos, sin)], 1
    )
    turn = angle(np.arange(half)[:, None] * outer[None, :], blocks)
    last = np.concatenate([np.cos(turn), -np.sin(turn)], 1)
    weight = np.full((blocks, LANES), 2.0 / length)
    weight[0, (lane % half == 0) & (group // 2 == 0)] = 1.0 / length
    return [np.asarray(t, np.float32) for t in (first, twiddle, second, third, last, weight)]


def dot(a, b, contract=(1, 0)):
    return lax.dot_general(
        a,
        b,
        (((contract[0],), (contract[1],)), ((), ())),
        precision=HIGHEST,
        preferred_element_type=jnp.float32,
    )


def peer_of(me, d, owners):
    if owners & (owners - 1):
        return lax.rem(me + d, owners)
    bit = 1
    peer = me
    while bit < owners:
        if d & bit:
            peer = peer + bit * (1 - 2 * lax.rem(lax.div(me, bit), 2))
        bit *= 2
    return peer


def kernel(
    dims,
    counts_hbm,
    moment_hbm,
    rupture_hbm,
    source_hbm,
    owner_hbm,
    slab_hbm,
    sgt_hbm,
    slip_hbm,
    first_hbm,
    twiddle_hbm,
    second_hbm,
    third_hbm,
    last_hbm,
    weight_hbm,
    out_ref,
    counts_ref,
    moment_ref,
    rupture_ref,
    source_ref,
    owner_ref,
    slab_ref,
    sgt_ref,
    slip_ref,
    first_ref,
    twiddle_ref,
    second_ref,
    third_ref,
    last_ref,
    weight_ref,
    meta_ref,
    slabs_ref,
    spect_ref,
    acc_ref,
    mine_ref,
    pair_ref,
    sums_ref,
    ring_ref,
    load_sem,
    meta_send,
    meta_recv,
    pair_send,
    pair_recv,
    ring_send,
    ring_recv,
):
    owners, variants, cores, lanes_q, delays, tail_block, tail_rows = dims
    moments, comps, slab_dev, samples = sgt_ref.shape
    ruptures = counts_ref.shape[1]
    rp_dev = moment_ref.shape[1]
    nrp = slab_ref.shape[1]
    functions = slip_ref.shape[0]
    half = samples // LANES
    blocks = 2 * half
    nv = owners * cores
    codes = ceil_to(ruptures, 3) // 3
    me = lax.axis_index("pts")
    my_var = lax.axis_index("var")
    my_core = lax.axis_index("cmp")
    peers = [peer_of(me, d, owners) for d in range(owners)]

    barrier = pltpu.get_barrier_semaphore()
    for d in range(1, owners):
        pl.semaphore_signal(
            barrier, inc=1, device_id={"pts": peers[d]}, device_id_type=MESH
        )
    for c in range(1, cores):
        pl.semaphore_signal(
            barrier, inc=1, device_id={"cmp": lax.rem(my_core + c, cores)}, device_id_type=MESH
        )
    loads = []
    for i, (src, dst) in enumerate(
        (
            (counts_hbm, counts_ref),
            (moment_hbm, moment_ref),
            (owner_hbm, owner_ref),
            (rupture_hbm, rupture_ref),
            (source_hbm, source_ref),
            (slab_hbm, slab_ref),
            (sgt_hbm, sgt_ref),
            (slip_hbm, slip_ref),
            (weight_hbm, weight_ref),
            (first_hbm, first_ref),
            (twiddle_hbm, twiddle_ref),
            (second_hbm, second_ref),
            (third_hbm, third_ref),
            (last_hbm, last_ref),
        )
    ):
        copy = pltpu.make_async_copy(src, dst, load_sem.at[i])
        copy.start()
        loads.append(copy)

    lane = lax.broadcasted_iota(jnp.int32, (1, lanes_q), 1)
    start = me * rp_dev
    slot = lane - start
    inside = (slot >= 0) & (slot < rp_dev)
    zero = jnp.zeros((1, lanes_q), jnp.float32)
    meta_ref[0] = jnp.zeros(meta_ref.shape[1:], jnp.float32)
    slabs_ref[...] = jnp.full(slabs_ref.shape, -1, jnp.int32)
    loads[0].wait()
    loads[1].wait()
    for j in range(moments):
        row = zero
        for l in range(rp_dev):
            row = jnp.where(slot == l, moment_ref[j, l], row)
        meta_ref[0, j : j + 1, :] = row
    total = jnp.int32(0)
    rup_row = jnp.zeros((1, lanes_q), jnp.int32)
    begin_row = jnp.zeros((1, lanes_q), jnp.int32)
    code = [jnp.int32(0)] * codes
    for r in range(ruptures):
        count = counts_ref[0, r]
        total = total + count
        passed = total <= slot
        rup_row = rup_row + passed.astype(jnp.int32)
        begin_row = jnp.where(passed, total, begin_row)
        code[r // 3] = code[r // 3] + count * 256 ** (r % 3)
    for g in range(codes):
        value = code[g].astype(jnp.float32)
        row = moments + 1 + 2 * g
        meta_ref[0, row : row + 1, :] = jnp.where(lane >= start + rp_dev, value, 0.0)
        meta_ref[0, row + 1 : row + 2, :] = zero + value
    meta_ref[0, moments : moments + 1, :] = jnp.where(
        inside, (rup_row + 256 * (slot - begin_row)).astype(jnp.float32), 0.0
    )

    pl.semaphore_wait(barrier, owners + cores - 2)
    order = list(range(owners - 1, 0, -1))
    metas = []
    for d in order:
        copy = pltpu.make_async_remote_copy(
            src_ref=meta_ref.at[0],
            dst_ref=meta_ref.at[d],
            send_sem=meta_send.at[d],
            recv_sem=meta_recv.at[d],
            device_id={"pts": peers[d]},
            device_id_type=MESH,
        )
        copy.start()
        metas.append(copy)

    for copy in loads[2:6]:
        copy.wait()
    slabs_ref[:, :nrp] = slab_ref[...]
    rup_v = jnp.zeros((nv, lanes_q), jnp.float32)
    src_v = jnp.zeros((nv, lanes_q), jnp.float32)
    v_iota = lax.broadcasted_iota(jnp.int32, (nv, lanes_q), 0)
    my_slip = jnp.int32(0)
    for i in range(nv):
        c = lax.rem(my_core + i // owners, cores)
        var_id = owner_ref[(peers[i % owners] * variants + my_var) * cores + c]
        rup_v = jnp.where(v_iota == i, rupture_ref[var_id].astype(jnp.float32), rup_v)
        src_v = jnp.where(v_iota == i, source_ref[0, var_id].astype(jnp.float32), src_v)
        if i == 0:
            my_slip = source_ref[1, var_id]

    loads[6].wait()
    for copy in metas:
        copy.wait()
    merged = meta_ref[0]
    for d in range(1, owners):
        merged = merged + meta_ref[d]
    mixed = merged[moments : moments + 1]
    pos_row = jnp.floor(mixed * (1.0 / 256))
    rup_row = mixed - 256.0 * pos_row
    len_v = jnp.zeros((nv, lanes_q), jnp.float32)
    rest = None
    for r in range(ruptures):
        if r % 3 == 0:
            row = moments + 1 + 2 * (r // 3)
            rest = merged[row : row + 2]
        above = jnp.floor(rest * (1.0 / 256))
        digit = rest - 256.0 * above
        rest = above
        pos_row = pos_row + jnp.where(rup_row == r, digit[0:1], 0.0)
        len_v = len_v + jnp.where(rup_v == r, digit[1:2], 0.0)
    hyp_v = jnp.floor((src_v * len_v + 0.5) * (1.0 / functions))
    apart = jnp.where(rup_v == rup_row, jnp.abs(pos_row - hyp_v), -1.0)
    local = slabs_ref[...] - me * slab_dev
    s_iota = lax.broadcasted_iota(jnp.int32, (slab_dev, lanes_q), 0)
    hit = s_iota == local
    spread = jnp.concatenate(
        [jnp.where(hit, merged[j : j + 1], 0.0) for j in range(moments)] * 2, axis=0
    )
    depth = moments * slab_dev
    upper = lax.broadcasted_iota(jnp.int32, (1, 2 * depth), 1) < depth
    group = delays
    while group * nv > 64 and group % 2 == 0:
        group //= 2
    groups = delays // group
    tail = tail_rows * LANES

    def weights_of(base):
        picks = jnp.concatenate(
            [
                (apart == jnp.float32(delta) + base).astype(jnp.float32)
                for delta in range(group)
            ],
            axis=0,
        )
        weights = dot(picks, spread, (1, 1))
        coarse = weights.astype(jnp.bfloat16).astype(jnp.float32)
        return jnp.where(upper, coarse, weights - coarse).astype(jnp.bfloat16)

    def gathered(pieces, c, begin, acc):
        series = jnp.concatenate([sgt_ref[j, c, :, begin:] for j in range(moments)] * 2, axis=0)
        product = jnp.dot(pieces, series, preferred_element_type=jnp.float32)
        pad = jnp.zeros((nv, tail), jnp.float32)
        for delta in reversed(range(group)):
            term = jnp.concatenate([product[delta * nv : (delta + 1) * nv], pad], axis=1)
            acc = term if acc is None else pltpu.roll(acc, TAU, 1) + term
        return acc

    def offset(c, i, n):
        return i * (tail_block + half) if c == 0 else n * (tail_block + c * half) + i * half

    def rows(c):
        return tail_block + half if c == 0 else half

    def put(c, row, tile):
        for b in range(nv // 8):
            mine_ref[pl.ds(offset(c, b * 8, nv) + row, 8, stride=rows(c)), :] = tile[
                b * 8 : (b + 1) * 8
            ]

    def emit_tail(c, acc, at):
        for e in range(tail_rows):
            put(0, e * comps + c, acc[:, at + e * LANES : at + (e + 1) * LANES])

    def emit(c, acc):
        for t1 in range(half):
            put(c, t1 + (tail_block if c == 0 else 0), acc[:, t1 * LANES : (t1 + 1) * LANES])

    def send_pair(c):
        copies = []
        for k in range(1, cores):
            copy = pltpu.make_async_remote_copy(
                src_ref=mine_ref.at[pl.ds(offset(c, k * owners, nv), owners * rows(c))],
                dst_ref=pair_ref.at[k - 1, pl.ds(offset(c, 0, owners), owners * rows(c))],
                send_sem=pair_send.at[c, k - 1],
                recv_sem=pair_recv.at[c, k - 1],
                device_id={"cmp": lax.rem(my_core + k, cores)},
                device_id_type=MESH,
            )
            copy.start()
            copies.append(copy)
        return copies

    def joined(c, d):
        at = offset(c, d, nv)
        value = mine_ref[at : at + rows(c), :]
        at = offset(c, d, owners)
        for k in range(1, cores):
            value = value + pair_ref[k - 1, at : at + rows(c), :]
        return value

    def place(c):
        return 0 if c == 0 else tail_block + c * half

    def send_ring(c):
        for copy in pairs[c]:
            copy.wait_recv()
        for d in order:
            sums_ref[d - 1, place(c) : place(c) + rows(c), :] = joined(c, d)
        copies = []
        for d in order:
            copy = pltpu.make_async_remote_copy(
                src_ref=sums_ref.at[d - 1, pl.ds(place(c), rows(c))],
                dst_ref=ring_ref.at[d - 1, pl.ds(place(c), rows(c))],
                send_sem=ring_send.at[c, d - 1],
                recv_sem=ring_recv.at[c, d - 1],
                device_id={"pts": peers[d]},
                device_id_type=MESH,
            )
            copy.start()
            copies.append(copy)
        return copies

    for i in range(nv):
        at = offset(0, i, nv)
        mine_ref[at : at + tail_block, :] = jnp.zeros((tail_block, LANES), jnp.float32)
    pairs, rings = [], []
    if groups > 1:
        acc_ref[...] = jnp.zeros(acc_ref.shape, jnp.float32)

        def one_group(step, carry):
            base = lax.convert_element_type((groups - 1 - step) * group, jnp.float32)
            pieces = weights_of(base)
            for c in range(comps):
                acc_ref[c] = gathered(pieces, c, 0, acc_ref[c])
            return carry

        lax.fori_loop(0, groups, one_group, 0)
        for c in range(comps):
            emit_tail(c, acc_ref[c], samples)
        for c in range(comps):
            emit(c, acc_ref[c])
            pairs.append(send_pair(c))
        for c in range(comps):
            rings.append(send_ring(c))
    else:
        pieces = weights_of(0.0)
        for c in range(comps):
            emit_tail(c, gathered(pieces, c, samples - tail, None), tail)
        for c in range(comps):
            emit(c, gathered(pieces, c, 0, None))
            pairs.append(send_pair(c))
            if c > 0:
                rings.append(send_ring(c - 1))
        rings.append(send_ring(comps - 1))

    loads[7].wait()
    for a in range(half):
        real = slip_ref[my_slip, 0:1, a * LANES : (a + 1) * LANES]
        imag = slip_ref[my_slip, 1:2, a * LANES : (a + 1) * LANES]
        spect_ref[a : a + 1, :] = real
        spect_ref[half + a : half + a + 1, :] = real
        spect_ref[2 * half + a : 2 * half + a + 1, :] = -imag
        spect_ref[3 * half + a : 3 * half + a + 1, :] = imag
    turned = jnp.transpose(spect_ref[...])
    for copy in loads[8:]:
        copy.wait()
    slip_real = weight_ref[...] * jnp.concatenate(
        [turned[:blocks, :blocks], turned[blocks:, :blocks]], axis=1
    )
    slip_imag = weight_ref[...] * jnp.concatenate(
        [turned[:blocks, blocks:], turned[blocks:, blocks:]], axis=1
    )
    cos, sin = twiddle_ref[0], twiddle_ref[1]
    tails = None
    for c in range(comps):
        packed = joined(c, 0)
        for copy in rings[c]:
            copy.wait_recv()
        for d in range(1, owners):
            packed = packed + ring_ref[d - 1, place(c) : place(c) + rows(c), :]
        if c == 0:
            tails = packed[:tail_block]
        else:
            packed = jnp.concatenate([tails, packed], axis=0)
        stage = dot(first_ref[c], packed)
        real, imag = stage[:blocks], stage[blocks:]
        turn = jnp.concatenate([real * cos + imag * sin, imag * cos - real * sin], axis=1)
        spectra = dot(turn, second_ref[...])
        spectra = spectra[:, :LANES] * slip_real + spectra[:, LANES:] * slip_imag
        middle = dot(spectra, third_ref[...])
        real, imag = middle[:, :LANES], middle[:, LANES:]
        turn = jnp.concatenate([real * cos - imag * sin, real * sin + imag * cos], axis=0)
        out_ref[c] = dot(last_ref[...], turn)
    for copies in pairs + rings:
        for copy in copies:
            copy.wait_send()


def per_device(owners, variants, cores, *args):
    sgt, moment, slip_spec, rp_slab, rup_counts, var_rupture, var_source, owner_map = args
    moments, comps, slab_dev, samples = sgt.shape
    nrp = rp_slab.shape[0]
    half = samples // LANES
    nv = owners * cores
    assert owner_map.shape[0] == nv * variants and 4 * half == LANES and nv % 8 == 0
    assert MOST * owners < 256 and moments + 1 + 2 * (ceil_to(rup_counts.shape[1], 3) // 3) <= 8
    lanes_q = ceil_to(nrp, LANES)
    delays = MOST * owners
    tail_rows = ceil_to(TAU * (delays - 1), LANES) // LANES
    width = samples + tail_rows * LANES
    tail_block = ceil_to(comps * tail_rows, 8)
    pitch = tail_block + comps * half
    consts = tables(comps, samples, tail_rows, tail_block)
    dims = (owners, variants, cores, lanes_q, delays, tail_block, tail_rows)
    f32 = jnp.float32
    others = max(owners - 1, 1)
    vmem = pl.BlockSpec(memory_space=pltpu.VMEM)
    anywhere = pl.BlockSpec(memory_space=pl.ANY)
    out = pl.pallas_call(
        functools.partial(kernel, dims),
        out_shape=jax.ShapeDtypeStruct((comps, half, LANES), f32),
        in_specs=[anywhere] * 14,
        out_specs=vmem,
        scratch_shapes=[
            pltpu.SMEM(rup_counts.shape, jnp.int32),
            pltpu.SMEM(moment.shape, f32),
            pltpu.SMEM(var_rupture.shape, jnp.int32),
            pltpu.SMEM(var_source.shape[::-1], jnp.int32),
            pltpu.SMEM(owner_map.shape, jnp.int32),
            pltpu.VMEM((1, nrp), jnp.int32),
            pltpu.VMEM(sgt.shape, sgt.dtype),
            pltpu.VMEM(slip_spec.shape, f32),
            *[pltpu.VMEM(t.shape, f32) for t in consts],
            pltpu.VMEM((owners, 8, lanes_q), f32),
            pltpu.VMEM((1, lanes_q), jnp.int32),
            pltpu.VMEM((LANES, LANES), f32),
            pltpu.VMEM((comps, nv, width) if nv * delays > 64 else (1, 8, LANES), f32),
            pltpu.VMEM((nv * pitch, LANES), f32),
            pltpu.VMEM((cores - 1, owners * pitch, LANES), f32),
            pltpu.VMEM((others, pitch, LANES), f32),
            pltpu.VMEM((others, pitch, LANES), f32),
            pltpu.SemaphoreType.DMA((14,)),
            pltpu.SemaphoreType.DMA((owners,)),
            pltpu.SemaphoreType.DMA((owners,)),
            pltpu.SemaphoreType.DMA((comps, cores)),
            pltpu.SemaphoreType.DMA((comps, cores)),
            pltpu.SemaphoreType.DMA((comps, owners)),
            pltpu.SemaphoreType.DMA((comps, owners)),
        ],
        compiler_params=pltpu.CompilerParams(collective_id=0, has_side_effects=True),
    )(
        rup_counts,
        moment,
        var_rupture,
        var_source.T,
        owner_map,
        rp_slab.reshape(1, nrp),
        sgt,
        slip_spec,
        *[jnp.asarray(t) for t in consts],
    )
    return out.reshape(1, comps, samples)


def solution(mesh):
    placed = (
        P("cmp", None, ("site", "pts"), None),
        P("cmp", ("site", "pts")),
        P(),
        P("site"),
        P(("site", "pts"), None),
        P("site"),
        P("site", None),
        P("site"),
    )
    sizes = (mesh.shape["pts"], mesh.shape["var"], mesh.shape["cmp"])
    return jax.shard_map(
        functools.partial(per_device, *sizes),
        mesh=mesh,
        in_specs=placed,
        out_specs=P(("site", "pts", "var", "cmp"), None, None),
        check_vma=False,
    )
```

```python
import functools
import math

import jax
import jax.numpy as jnp
import numpy as np
from jax import lax
from jax.experimental import pallas as pl
from jax.experimental.pallas import tpu as pltpu
from jax.sharding import PartitionSpec as P

TAU = 4
MOST = 2
LANES = 128
MESH = pl.DeviceIdType.MESH
HIGHEST = lax.Precision.HIGHEST


def ceil_to(value, unit):
    return (value + unit - 1) // unit * unit


def tables(comps, samples, tail_rows, tail_block):
    length = 2 * samples
    blocks = length // LANES
    half = blocks // 2
    outer = np.arange(blocks)

    def angle(numer, period):
        return 2.0 * np.pi * (numer % period) / period

    first = np.zeros((comps, 2 * blocks, tail_block + half))
    for c in range(comps):
        for t1 in range(half + tail_rows):
            row = tail_block + t1 if t1 < half else (t1 - half) * comps + c
            turn = angle(outer * t1, blocks)
            first[c, :blocks, row] = np.cos(turn)
            first[c, blocks:, row] = -np.sin(turn)
    lane = np.arange(LANES)
    turn = angle(outer[:, None] * lane[None, :], length)
    twiddle = np.stack([np.cos(turn), np.sin(turn)])
    group = lane // half
    k2 = 2 * (lane % half) + group // 2
    imag = group % 2
    turn = angle(lane[:, None] * k2[None, :], LANES)
    cos, sin = np.cos(turn), np.sin(turn)
    top = np.where(imag[None] == 1, -sin, cos)
    bottom = np.where(imag[None] == 1, cos, sin)
    top_swap = np.where(imag[None] == 0, -sin, cos)
    bottom_swap = np.where(imag[None] == 0, cos, sin)
    second = np.concatenate(
        [np.concatenate([top, top_swap], 1), np.concatenate([bottom, bottom_swap], 1)], 0
    )
    turn = angle(k2[:, None] * lane[None, :], LANES)
    cos, sin = np.cos(turn), np.sin(turn)
    third = np.concatenate(
        [np.where(imag[:, None] == 1, -sin, cos), np.where(imag[:, None] == 1, cos, sin)], 1
    )
    turn = angle(np.arange(half)[:, None] * outer[None, :], blocks)
    last = np.concatenate([np.cos(turn), -np.sin(turn)], 1)
    weight = np.full((blocks, LANES), 2.0 / length)
    weight[0, (lane % half == 0) & (group // 2 == 0)] = 1.0 / length

    def pieces(table, axis=0):
        coarse = table.astype(jnp.bfloat16)
        return np.stack([coarse, (table - coarse.astype(np.float64)).astype(jnp.bfloat16)], axis)

    return [
        pieces(first, 1),
        twiddle.astype(np.float32),
        pieces(second),
        pieces(third),
        pieces(last),
        weight.astype(np.float32),
    ]


def dot(a, b, contract=(1, 0)):
    return lax.dot_general(
        a,
        b,
        (((contract[0],), (contract[1],)), ((), ())),
        precision=HIGHEST,
        preferred_element_type=jnp.float32,
    )


def halves(value):
    coarse = value.astype(jnp.bfloat16)
    return coarse, (value - coarse.astype(jnp.float32)).astype(jnp.bfloat16)


def right(a, table):
    coarse, fine = halves(a)
    big, small = table[0], table[1]
    return (
        jnp.dot(coarse, small, preferred_element_type=jnp.float32)
        + jnp.dot(fine, big, preferred_element_type=jnp.float32)
        + jnp.dot(coarse, big, preferred_element_type=jnp.float32)
    )


def left(table, b):
    coarse, fine = halves(b)
    big, small = table[0], table[1]
    return (
        jnp.dot(small, coarse, preferred_element_type=jnp.float32)
        + jnp.dot(big, fine, preferred_element_type=jnp.float32)
        + jnp.dot(big, coarse, preferred_element_type=jnp.float32)
    )


def peer_of(me, d, owners):
    if owners & (owners - 1):
        return lax.rem(me + d, owners)
    bit = 1
    peer = me
    while bit < owners:
        if d & bit:
            peer = peer + bit * (1 - 2 * lax.rem(lax.div(me, bit), 2))
        bit *= 2
    return peer


def kernel(
    dims,
    counts_hbm,
    moment_hbm,
    rupture_hbm,
    source_hbm,
    owner_hbm,
    slab_hbm,
    sgt_hbm,
    slip_hbm,
    first_hbm,
    twiddle_hbm,
    second_hbm,
    third_hbm,
    last_hbm,
    weight_hbm,
    out_ref,
    counts_ref,
    moment_ref,
    rupture_ref,
    source_ref,
    owner_ref,
    slab_ref,
    sgt_ref,
    slip_ref,
    first_ref,
    twiddle_ref,
    second_ref,
    third_ref,
    last_ref,
    weight_ref,
    meta_ref,
    slabs_ref,
    spect_ref,
    acc_ref,
    mine_ref,
    pair_ref,
    sums_ref,
    ring_ref,
    load_sem,
    meta_send,
    meta_recv,
    pair_send,
    pair_recv,
    ring_send,
    ring_recv,
):
    owners, variants, cores, lanes_q, delays, tail_block, tail_rows = dims
    moments, comps, slab_dev, samples = sgt_ref.shape
    ruptures = counts_ref.shape[1]
    rp_dev = moment_ref.shape[1]
    nrp = slab_ref.shape[1]
    functions = slip_ref.shape[0]
    half = samples // LANES
    blocks = 2 * half
    nv = owners * cores
    codes = ceil_to(ruptures, 3) // 3
    me = lax.axis_index("pts")
    my_var = lax.axis_index("var")
    my_core = lax.axis_index("cmp")
    peers = [peer_of(me, d, owners) for d in range(owners)]

    barrier = pltpu.get_barrier_semaphore()
    for d in range(1, owners):
        pl.semaphore_signal(
            barrier, inc=1, device_id={"pts": peers[d]}, device_id_type=MESH
        )
    for c in range(1, cores):
        pl.semaphore_signal(
            barrier, inc=1, device_id={"cmp": lax.rem(my_core + c, cores)}, device_id_type=MESH
        )
    loads = []
    for i, (src, dst) in enumerate(
        (
            (counts_hbm, counts_ref),
            (moment_hbm, moment_ref),
            (owner_hbm, owner_ref),
            (rupture_hbm, rupture_ref),
            (source_hbm, source_ref),
            (slab_hbm, slab_ref),
            (sgt_hbm, sgt_ref),
            (slip_hbm, slip_ref),
            (weight_hbm, weight_ref),
            (first_hbm, first_ref),
            (twiddle_hbm, twiddle_ref),
            (second_hbm, second_ref),
            (third_hbm, third_ref),
            (last_hbm, last_ref),
        )
    ):
        copy = pltpu.make_async_copy(src, dst, load_sem.at[i])
        copy.start()
        loads.append(copy)

    lane = lax.broadcasted_iota(jnp.int32, (1, lanes_q), 1)
    start = me * rp_dev
    slot = lane - start
    inside = (slot >= 0) & (slot < rp_dev)
    zero = jnp.zeros((1, lanes_q), jnp.float32)
    meta_ref[0] = jnp.zeros(meta_ref.shape[1:], jnp.float32)
    slabs_ref[...] = jnp.full(slabs_ref.shape, -1, jnp.int32)
    loads[0].wait()
    loads[1].wait()
    for j in range(moments):
        row = zero
        for l in range(rp_dev):
            row = jnp.where(slot == l, moment_ref[j, l], row)
        meta_ref[0, j : j + 1, :] = row
    total = jnp.int32(0)
    rup_row = jnp.zeros((1, lanes_q), jnp.int32)
    begin_row = jnp.zeros((1, lanes_q), jnp.int32)
    code = [jnp.int32(0)] * codes
    for r in range(ruptures):
        count = counts_ref[0, r]
        total = total + count
        passed = total <= slot
        rup_row = rup_row + passed.astype(jnp.int32)
        begin_row = jnp.where(passed, total, begin_row)
        code[r // 3] = code[r // 3] + count * 256 ** (r % 3)
    for g in range(codes):
        value = code[g].astype(jnp.float32)
        row = moments + 1 + 2 * g
        meta_ref[0, row : row + 1, :] = jnp.where(lane >= start + rp_dev, value, 0.0)
        meta_ref[0, row + 1 : row + 2, :] = zero + value
    meta_ref[0, moments : moments + 1, :] = jnp.where(
        inside, (rup_row + 256 * (slot - begin_row)).astype(jnp.float32), 0.0
    )

    pl.semaphore_wait(barrier, owners + cores - 2)
    order = list(range(owners - 1, 0, -1))
    metas = []
    for d in order:
        copy = pltpu.make_async_remote_copy(
            src_ref=meta_ref.at[0],
            dst_ref=meta_ref.at[d],
            send_sem=meta_send.at[d],
            recv_sem=meta_recv.at[d],
            device_id={"pts": peers[d]},
            device_id_type=MESH,
        )
        copy.start()
        metas.append(copy)

    for copy in loads[2:6]:
        copy.wait()
    slabs_ref[:, :nrp] = slab_ref[...]
    rup_v = jnp.zeros((nv, lanes_q), jnp.float32)
    src_v = jnp.zeros((nv, lanes_q), jnp.float32)
    v_iota = lax.broadcasted_iota(jnp.int32, (nv, lanes_q), 0)
    my_slip = jnp.int32(0)
    for i in range(nv):
        c = lax.rem(my_core + i // owners, cores)
        var_id = owner_ref[(peers[i % owners] * variants + my_var) * cores + c]
        rup_v = jnp.where(v_iota == i, rupture_ref[var_id].astype(jnp.float32), rup_v)
        src_v = jnp.where(v_iota == i, source_ref[0, var_id].astype(jnp.float32), src_v)
        if i == 0:
            my_slip = source_ref[1, var_id]

    loads[6].wait()
    for copy in metas:
        copy.wait()
    merged = meta_ref[0]
    for d in range(1, owners):
        merged = merged + meta_ref[d]
    mixed = merged[moments : moments + 1]
    pos_row = jnp.floor(mixed * (1.0 / 256))
    rup_row = mixed - 256.0 * pos_row
    len_v = jnp.zeros((nv, lanes_q), jnp.float32)
    rest = None
    for r in range(ruptures):
        if r % 3 == 0:
            row = moments + 1 + 2 * (r // 3)
            rest = merged[row : row + 2]
        above = jnp.floor(rest * (1.0 / 256))
        digit = rest - 256.0 * above
        rest = above
        pos_row = pos_row + jnp.where(rup_row == r, digit[0:1], 0.0)
        len_v = len_v + jnp.where(rup_v == r, digit[1:2], 0.0)
    hyp_v = jnp.floor((src_v * len_v + 0.5) * (1.0 / functions))
    apart = jnp.where(rup_v == rup_row, jnp.abs(pos_row - hyp_v), -1.0)
    local = slabs_ref[...] - me * slab_dev
    s_iota = lax.broadcasted_iota(jnp.int32, (slab_dev, lanes_q), 0)
    hit = s_iota == local
    spread = jnp.concatenate(
        [jnp.where(hit, merged[j : j + 1], 0.0) for j in range(moments)] * 2, axis=0
    )
    depth = moments * slab_dev
    upper = lax.broadcasted_iota(jnp.int32, (1, 2 * depth), 1) < depth
    group = delays
    while group * nv > 64 and group % 2 == 0:
        group //= 2
    groups = delays // group
    tail = tail_rows * LANES

    def weights_of(base):
        picks = jnp.concatenate(
            [
                (apart == jnp.float32(delta) + base).astype(jnp.float32)
                for delta in range(group)
            ],
            axis=0,
        )
        weights = dot(picks, spread, (1, 1))
        coarse = weights.astype(jnp.bfloat16).astype(jnp.float32)
        return jnp.where(upper, coarse, weights - coarse).astype(jnp.bfloat16)

    def gathered(pieces, c, begin, acc):
        series = jnp.concatenate([sgt_ref[j, c, :, begin:] for j in range(moments)] * 2, axis=0)
        product = jnp.dot(pieces, series, preferred_element_type=jnp.float32)
        pad = jnp.zeros((nv, tail), jnp.float32)
        for delta in reversed(range(group)):
            term = jnp.concatenate([product[delta * nv : (delta + 1) * nv], pad], axis=1)
            acc = term if acc is None else pltpu.roll(acc, TAU, 1) + term
        return acc

    def offset(c, i, n):
        return i * (tail_block + half) if c == 0 else n * (tail_block + c * half) + i * half

    def rows(c):
        return tail_block + half if c == 0 else half

    def put(c, row, tile):
        for b in range(nv // 8):
            mine_ref[pl.ds(offset(c, b * 8, nv) + row, 8, stride=rows(c)), :] = tile[
                b * 8 : (b + 1) * 8
            ]

    def emit_tail(c, acc, at):
        for e in range(tail_rows):
            put(0, e * comps + c, acc[:, at + e * LANES : at + (e + 1) * LANES])

    def emit(c, acc):
        for t1 in range(half):
            put(c, t1 + (tail_block if c == 0 else 0), acc[:, t1 * LANES : (t1 + 1) * LANES])

    def send_pair(c):
        copies = []
        for k in range(1, cores):
            copy = pltpu.make_async_remote_copy(
                src_ref=mine_ref.at[pl.ds(offset(c, k * owners, nv), owners * rows(c))],
                dst_ref=pair_ref.at[k - 1, pl.ds(offset(c, 0, owners), owners * rows(c))],
                send_sem=pair_send.at[c, k - 1],
                recv_sem=pair_recv.at[c, k - 1],
                device_id={"cmp": lax.rem(my_core + k, cores)},
                device_id_type=MESH,
            )
            copy.start()
            copies.append(copy)
        return copies

    def joined(c, d):
        at = offset(c, d, nv)
        value = mine_ref[at : at + rows(c), :]
        at = offset(c, d, owners)
        for k in range(1, cores):
            value = value + pair_ref[k - 1, at : at + rows(c), :]
        return value

    def place(c):
        return 0 if c == 0 else tail_block + c * half

    def send_ring(c):
        for copy in pairs[c]:
            copy.wait_recv()
        for d in order:
            sums_ref[d - 1, place(c) : place(c) + rows(c), :] = joined(c, d)
        copies = []
        for d in order:
            copy = pltpu.make_async_remote_copy(
                src_ref=sums_ref.at[d - 1, pl.ds(place(c), rows(c))],
                dst_ref=ring_ref.at[d - 1, pl.ds(place(c), rows(c))],
                send_sem=ring_send.at[c, d - 1],
                recv_sem=ring_recv.at[c, d - 1],
                device_id={"pts": peers[d]},
                device_id_type=MESH,
            )
            copy.start()
            copies.append(copy)
        return copies

    for i in range(nv):
        at = offset(0, i, nv)
        mine_ref[at : at + tail_block, :] = jnp.zeros((tail_block, LANES), jnp.float32)
    pairs, rings = [], []
    if groups > 1:
        acc_ref[...] = jnp.zeros(acc_ref.shape, jnp.float32)

        def one_group(step, carry):
            base = lax.convert_element_type((groups - 1 - step) * group, jnp.float32)
            pieces = weights_of(base)
            for c in range(comps):
                acc_ref[c] = gathered(pieces, c, 0, acc_ref[c])
            return carry

        lax.fori_loop(0, groups, one_group, 0)
        for c in range(comps):
            emit_tail(c, acc_ref[c], samples)
        for c in range(comps):
            emit(c, acc_ref[c])
            pairs.append(send_pair(c))
        for c in range(comps):
            rings.append(send_ring(c))
    else:
        pieces = weights_of(0.0)
        for c in range(comps):
            emit_tail(c, gathered(pieces, c, samples - tail, None), tail)
        for c in range(comps):
            emit(c, gathered(pieces, c, 0, None))
            pairs.append(send_pair(c))
        for c in range(comps):
            rings.append(send_ring(c))

    loads[7].wait()
    for a in range(half):
        real = slip_ref[my_slip, 0:1, a * LANES : (a + 1) * LANES]
        imag = slip_ref[my_slip, 1:2, a * LANES : (a + 1) * LANES]
        spect_ref[a : a + 1, :] = real
        spect_ref[half + a : half + a + 1, :] = real
        spect_ref[2 * half + a : 2 * half + a + 1, :] = -imag
        spect_ref[3 * half + a : 3 * half + a + 1, :] = imag
    turned = jnp.transpose(spect_ref[...])
    for copy in loads[8:]:
        copy.wait()
    slip_real = weight_ref[...] * jnp.concatenate(
        [turned[:blocks, :blocks], turned[blocks:, :blocks]], axis=1
    )
    slip_imag = weight_ref[...] * jnp.concatenate(
        [turned[:blocks, blocks:], turned[blocks:, blocks:]], axis=1
    )
    cos, sin = twiddle_ref[0], twiddle_ref[1]
    tails = None
    for c in range(comps):
        packed = joined(c, 0)
        for copy in rings[c]:
            copy.wait_recv()
        for d in range(1, owners):
            packed = packed + ring_ref[d - 1, place(c) : place(c) + rows(c), :]
        if c == 0:
            tails = packed[:tail_block]
        else:
            packed = jnp.concatenate([tails, packed], axis=0)
        stage = left(first_ref.at[c], packed)
        real, imag = stage[:blocks], stage[blocks:]
        turn = jnp.concatenate([real * cos + imag * sin, imag * cos - real * sin], axis=1)
        spectra = right(turn, second_ref)
        spectra = spectra[:, :LANES] * slip_real + spectra[:, LANES:] * slip_imag
        middle = right(spectra, third_ref)
        real, imag = middle[:, :LANES], middle[:, LANES:]
        turn = jnp.concatenate([real * cos - imag * sin, real * sin + imag * cos], axis=0)
        out_ref[c] = left(last_ref, turn)
    for copies in pairs + rings:
        for copy in copies:
            copy.wait_send()


def per_device(owners, variants, cores, *args):
    sgt, moment, slip_spec, rp_slab, rup_counts, var_rupture, var_source, owner_map = args
    moments, comps, slab_dev, samples = sgt.shape
    nrp = rp_slab.shape[0]
    half = samples // LANES
    nv = owners * cores
    assert owner_map.shape[0] == nv * variants and 4 * half == LANES and nv % 8 == 0
    assert MOST * owners < 256 and moments + 1 + 2 * (ceil_to(rup_counts.shape[1], 3) // 3) <= 8
    lanes_q = ceil_to(nrp, LANES)
    delays = MOST * owners
    tail_rows = ceil_to(TAU * (delays - 1), LANES) // LANES
    width = samples + tail_rows * LANES
    tail_block = ceil_to(comps * tail_rows, 8)
    pitch = tail_block + comps * half
    consts = tables(comps, samples, tail_rows, tail_block)
    dims = (owners, variants, cores, lanes_q, delays, tail_block, tail_rows)
    f32 = jnp.float32
    others = max(owners - 1, 1)
    vmem = pl.BlockSpec(memory_space=pltpu.VMEM)
    anywhere = pl.BlockSpec(memory_space=pl.ANY)
    out = pl.pallas_call(
        functools.partial(kernel, dims),
        out_shape=pltpu.VMEM((comps, half, LANES), f32),
        in_specs=[anywhere] * 14,
        out_specs=vmem,
        scratch_shapes=[
            pltpu.SMEM(rup_counts.shape, jnp.int32),
            pltpu.SMEM(moment.shape, f32),
            pltpu.SMEM(var_rupture.shape, jnp.int32),
            pltpu.SMEM(var_source.shape[::-1], jnp.int32),
            pltpu.SMEM(owner_map.shape, jnp.int32),
            pltpu.VMEM((1, nrp), jnp.int32),
            pltpu.VMEM(sgt.shape, sgt.dtype),
            pltpu.VMEM(slip_spec.shape, f32),
            *[pltpu.VMEM(t.shape, t.dtype) for t in consts],
            pltpu.VMEM((owners, 8, lanes_q), f32),
            pltpu.VMEM((1, lanes_q), jnp.int32),
            pltpu.VMEM((LANES, LANES), f32),
            pltpu.VMEM((comps, nv, width) if nv * delays > 64 else (1, 8, LANES), f32),
            pltpu.VMEM((nv * pitch, LANES), f32),
            pltpu.VMEM((cores - 1, owners * pitch, LANES), f32),
            pltpu.VMEM((others, pitch, LANES), f32),
            pltpu.VMEM((others, pitch, LANES), f32),
            pltpu.SemaphoreType.DMA((14,)),
            pltpu.SemaphoreType.DMA((owners,)),
            pltpu.SemaphoreType.DMA((owners,)),
            pltpu.SemaphoreType.DMA((comps, cores)),
            pltpu.SemaphoreType.DMA((comps, cores)),
            pltpu.SemaphoreType.DMA((comps, owners)),
            pltpu.SemaphoreType.DMA((comps, owners)),
        ],
        compiler_params=pltpu.CompilerParams(collective_id=0, has_side_effects=True),
    )(
        rup_counts,
        moment,
        var_rupture,
        var_source.T,
        owner_map,
        rp_slab.reshape(1, nrp),
        sgt,
        slip_spec,
        *[jnp.asarray(t) for t in consts],
    )
    return out.reshape(1, comps, samples)


def solution(mesh):
    placed = (
        P("cmp", None, ("site", "pts"), None),
        P("cmp", ("site", "pts")),
        P(),
        P("site"),
        P(("site", "pts"), None),
        P("site"),
        P("site", None),
        P("site"),
    )
    sizes = (mesh.shape["pts"], mesh.shape["var"], mesh.shape["cmp"])
    return jax.shard_map(
        functools.partial(per_device, *sizes),
        mesh=mesh,
        in_specs=placed,
        out_specs=P(("site", "pts", "var", "cmp"), None, None),
        check_vma=False,
    )
```

```python
import functools
import math

import jax
import jax.numpy as jnp
import numpy as np
from jax import lax
from jax.experimental import pallas as pl
from jax.experimental.pallas import tpu as pltpu
from jax.sharding import PartitionSpec as P

TAU = 4
MOST = 2
LANES = 128
MESH = pl.DeviceIdType.MESH
HIGHEST = lax.Precision.HIGHEST


def ceil_to(value, unit):
    return (value + unit - 1) // unit * unit


def tables(comps, samples, tail_rows, row_pitch):
    length = 2 * samples
    blocks = length // LANES
    half = blocks // 2
    outer = np.arange(blocks)

    def angle(numer, period):
        return 2.0 * np.pi * (numer % period) / period

    first = np.zeros((comps, 2 * blocks, row_pitch))
    for c in range(comps):
        for t1 in range(half + tail_rows):
            row = c * half + t1 if t1 < half else comps * half + (t1 - half) * comps + c
            turn = angle(outer * t1, blocks)
            first[c, :blocks, row] = np.cos(turn)
            first[c, blocks:, row] = -np.sin(turn)
    first = first.reshape(comps * 2 * blocks, row_pitch)
    lane = np.arange(LANES)
    turn = angle(outer[:, None] * lane[None, :], length)
    twiddle = np.stack([np.cos(turn), np.sin(turn)])
    group = lane // half
    k2 = 2 * (lane % half) + group // 2
    imag = group % 2
    turn = angle(lane[:, None] * k2[None, :], LANES)
    cos, sin = np.cos(turn), np.sin(turn)
    top = np.where(imag[None] == 1, -sin, cos)
    bottom = np.where(imag[None] == 1, cos, sin)
    top_swap = np.where(imag[None] == 0, -sin, cos)
    bottom_swap = np.where(imag[None] == 0, cos, sin)
    second = np.concatenate(
        [np.concatenate([top, top_swap], 1), np.concatenate([bottom, bottom_swap], 1)], 0
    )
    turn = angle(k2[:, None] * lane[None, :], LANES)
    cos, sin = np.cos(turn), np.sin(turn)
    third = np.concatenate(
        [np.where(imag[:, None] == 1, -sin, cos), np.where(imag[:, None] == 1, cos, sin)], 1
    )
    turn = angle(np.arange(half)[:, None] * outer[None, :], blocks)
    last = np.concatenate([np.cos(turn), -np.sin(turn)], 1)
    weight = np.full((blocks, LANES), 2.0 / length)
    weight[0, (lane % half == 0) & (group // 2 == 0)] = 1.0 / length
    def pieces(table, axis=0):
        coarse = table.astype(jnp.bfloat16)
        return np.stack([coarse, (table - coarse.astype(np.float64)).astype(jnp.bfloat16)], axis)

    return [
        pieces(first),
        twiddle.astype(np.float32),
        pieces(second),
        pieces(third),
        pieces(last),
        weight.astype(np.float32),
    ]


def dot(a, b, contract=(1, 0)):
    return lax.dot_general(
        a,
        b,
        (((contract[0],), (contract[1],)), ((), ())),
        precision=HIGHEST,
        preferred_element_type=jnp.float32,
    )


def halves(value):
    coarse = value.astype(jnp.bfloat16)
    return coarse, (value - coarse.astype(jnp.float32)).astype(jnp.bfloat16)


def right(a, table):
    coarse, fine = halves(a)
    big, small = table[0], table[1]
    return (
        jnp.dot(coarse, small, preferred_element_type=jnp.float32)
        + jnp.dot(fine, big, preferred_element_type=jnp.float32)
        + jnp.dot(coarse, big, preferred_element_type=jnp.float32)
    )


def left(table, b):
    coarse, fine = halves(b)
    big, small = table[0], table[1]
    return (
        jnp.dot(small, coarse, preferred_element_type=jnp.float32)
        + jnp.dot(big, fine, preferred_element_type=jnp.float32)
        + jnp.dot(big, coarse, preferred_element_type=jnp.float32)
    )


def kernel(
    dims,
    counts_ref,
    moment_ref,
    rupture_ref,
    source_ref,
    owner_ref,
    slab_ref,
    sgt_hbm,
    slip_hbm,
    first_hbm,
    twiddle_hbm,
    second_hbm,
    third_hbm,
    last_hbm,
    weight_hbm,
    out_ref,
    sgt_ref,
    slip_ref,
    first_ref,
    twiddle_ref,
    second_ref,
    third_ref,
    last_ref,
    weight_ref,
    meta_ref,
    slabs_ref,
    spect_ref,
    acc_ref,
    mine_ref,
    pair_ref,
    sums_ref,
    ring_ref,
    load_sem,
    meta_send,
    meta_recv,
    pair_send,
    pair_recv,
    ring_send,
    ring_recv,
):
    owners, variants, cores, lanes_q, delays, pitch, tail_rows = dims
    moments, comps, slab_dev, samples = sgt_ref.shape
    ruptures = counts_ref.shape[1]
    rp_dev = moment_ref.shape[1]
    nrp = slab_ref.shape[1]
    functions = slip_ref.shape[0]
    half = samples // LANES
    blocks = 2 * half
    nv = owners * cores
    me = lax.axis_index("pts")
    my_var = lax.axis_index("var")
    my_core = lax.axis_index("cmp")

    barrier = pltpu.get_barrier_semaphore()
    for d in range(1, owners):
        pl.semaphore_signal(
            barrier, inc=1, device_id={"pts": lax.rem(me + d, owners)}, device_id_type=MESH
        )
    for c in range(1, cores):
        pl.semaphore_signal(
            barrier, inc=1, device_id={"cmp": lax.rem(my_core + c, cores)}, device_id_type=MESH
        )
    loads = []
    for i, (src, dst) in enumerate(
        (
            (sgt_hbm, sgt_ref),
            (slip_hbm, slip_ref),
            (weight_hbm, weight_ref),
            (first_hbm, first_ref),
            (twiddle_hbm, twiddle_ref),
            (second_hbm, second_ref),
            (third_hbm, third_ref),
            (last_hbm, last_ref),
        )
    ):
        copy = pltpu.make_async_copy(src, dst, load_sem.at[i])
        copy.start()
        loads.append(copy)

    lane = lax.broadcasted_iota(jnp.int32, (1, lanes_q), 1)
    start = me * rp_dev
    slot = lane - start
    inside = (slot >= 0) & (slot < rp_dev)
    zero = jnp.zeros((1, lanes_q), jnp.float32)
    meta_ref[0] = jnp.zeros(meta_ref.shape[1:], jnp.float32)
    for j in range(moments):
        row = zero
        for l in range(rp_dev):
            row = jnp.where(slot == l, moment_ref[j, l], row)
        meta_ref[0, j : j + 1, :] = row
    total = jnp.int32(0)
    rup_row = jnp.zeros((1, lanes_q), jnp.int32)
    begin_row = jnp.zeros((1, lanes_q), jnp.int32)
    for r in range(ruptures):
        count = counts_ref[0, r]
        total = total + count
        passed = total <= slot
        rup_row = rup_row + passed.astype(jnp.int32)
        begin_row = jnp.where(passed, total, begin_row)
        value = count.astype(jnp.float32)
        meta_ref[0, 8 + r : 9 + r, :] = jnp.where(lane >= start + rp_dev, value, 0.0)
        meta_ref[0, 16 + r : 17 + r, :] = zero + value
    meta_ref[0, moments : moments + 1, :] = jnp.where(inside, rup_row.astype(jnp.float32), 0.0)
    meta_ref[0, moments + 1 : moments + 2, :] = jnp.where(
        inside, (slot - begin_row).astype(jnp.float32), 0.0
    )
    slabs_ref[...] = jnp.full(slabs_ref.shape, -1, jnp.int32)
    slabs_ref[:, :nrp] = slab_ref[...]

    rup_v = jnp.zeros((nv, lanes_q), jnp.float32)
    src_v = jnp.zeros((nv, lanes_q), jnp.float32)
    v_iota = lax.broadcasted_iota(jnp.int32, (nv, lanes_q), 0)
    my_slip = jnp.int32(0)
    for i in range(nv):
        p = lax.rem(me + i % owners, owners)
        c = lax.rem(my_core + i // owners, cores)
        var_id = owner_ref[(p * variants + my_var) * cores + c]
        rup_v = jnp.where(v_iota == i, rupture_ref[var_id].astype(jnp.float32), rup_v)
        src_v = jnp.where(v_iota == i, source_ref[0, var_id].astype(jnp.float32), src_v)
        if i == 0:
            my_slip = source_ref[1, var_id]

    pl.semaphore_wait(barrier, owners + cores - 2)
    metas = []
    for d in range(1, owners):
        copy = pltpu.make_async_remote_copy(
            src_ref=meta_ref.at[0],
            dst_ref=meta_ref.at[d],
            send_sem=meta_send.at[d],
            recv_sem=meta_recv.at[d],
            device_id={"pts": lax.rem(me + d, owners)},
            device_id_type=MESH,
        )
        copy.start()
        metas.append(copy)

    loads[0].wait()
    for copy in metas:
        copy.wait()
    merged = meta_ref[0]
    for d in range(1, owners):
        merged = merged + meta_ref[d]
    rup_row = merged[moments : moments + 1]
    pos_row = merged[moments + 1 : moments + 2]
    len_v = jnp.zeros((nv, lanes_q), jnp.float32)
    for r in range(ruptures):
        pos_row = pos_row + jnp.where(rup_row == r, merged[8 + r : 9 + r], 0.0)
        len_v = len_v + jnp.where(rup_v == r, merged[16 + r : 17 + r], 0.0)
    hyp_v = jnp.floor((src_v * len_v + 0.5) * (1.0 / functions))
    apart = jnp.where(rup_v == rup_row, jnp.abs(pos_row - hyp_v), -1.0)
    local = slabs_ref[...] - me * slab_dev
    s_iota = lax.broadcasted_iota(jnp.int32, (slab_dev, lanes_q), 0)
    hit = s_iota == local
    spread = jnp.concatenate(
        [jnp.where(hit, merged[j : j + 1], 0.0) for j in range(moments)] * 2, axis=0
    )
    depth = moments * slab_dev
    upper = lax.broadcasted_iota(jnp.int32, (1, 2 * depth), 1) < depth
    group = delays
    while group * nv > 64 and group % 2 == 0:
        group //= 2
    groups = delays // group
    width = samples + tail_rows * LANES
    if groups > 1:
        acc_ref[...] = jnp.zeros(acc_ref.shape, jnp.float32)

    def one_group(step, carry):
        base = (groups - 1 - step) * group
        picks = jnp.concatenate(
            [
                (apart == jnp.float32(delta) + lax.convert_element_type(base, jnp.float32)).astype(
                    jnp.float32
                )
                for delta in range(group)
            ],
            axis=0,
        )
        weights = dot(picks, spread, (1, 1))
        coarse = weights.astype(jnp.bfloat16)
        fine = (weights - coarse.astype(jnp.float32)).astype(jnp.bfloat16)
        pieces = jnp.where(upper, coarse.astype(jnp.float32), fine.astype(jnp.float32)).astype(
            jnp.bfloat16
        )
        pad = jnp.zeros((nv, width - samples), jnp.float32)
        for c in range(comps):
            series = jnp.concatenate([sgt_ref[j, c] for j in range(moments)] * 2, axis=0)
            product = jnp.dot(pieces, series, preferred_element_type=jnp.float32)
            acc = acc_ref[c] if groups > 1 else None
            for delta in reversed(range(group)):
                term = jnp.concatenate([product[delta * nv : (delta + 1) * nv], pad], axis=1)
                acc = term if acc is None else pltpu.roll(acc, TAU, 1) + term
            if groups > 1:
                acc_ref[c] = acc
            else:
                emit(c, acc)
        return carry

    def emit(c, acc):
        for t1 in range(half + tail_rows):
            row = c * half + t1 if t1 < half else comps * half + (t1 - half) * comps + c
            for b in range(nv // 8):
                mine_ref[pl.ds(b * 8 * pitch + row, 8, stride=pitch), :] = acc[
                    b * 8 : (b + 1) * 8, t1 * LANES : (t1 + 1) * LANES
                ]

    used = comps * (half + tail_rows)
    for i in range(nv):
        if used < pitch:
            mine_ref[i * pitch + used : (i + 1) * pitch, :] = jnp.zeros(
                (pitch - used, LANES), jnp.float32
            )
    if groups > 1:
        lax.fori_loop(0, groups, one_group, 0)
        for c in range(comps):
            emit(c, acc_ref[c])
    else:
        one_group(0, 0)

    size = owners * pitch
    pairs = []
    for c in range(1, cores):
        copy = pltpu.make_async_remote_copy(
            src_ref=mine_ref.at[pl.ds(c * size, size)],
            dst_ref=pair_ref.at[c - 1],
            send_sem=pair_send.at[c - 1],
            recv_sem=pair_recv.at[c - 1],
            device_id={"cmp": lax.rem(my_core + c, cores)},
            device_id_type=MESH,
        )
        copy.start()
        pairs.append(copy)
    for copy in pairs:
        copy.wait_recv()
    order = sorted(range(1, owners), key=lambda d: -min(d, owners - d))

    def joined(d):
        value = mine_ref[d * pitch : (d + 1) * pitch, :]
        for c in range(1, cores):
            value = value + pair_ref[c - 1, d * pitch : (d + 1) * pitch, :]
        return value

    for d in order:
        sums_ref[d - 1] = joined(d)
    rings = []
    for d in order:
        copy = pltpu.make_async_remote_copy(
            src_ref=sums_ref.at[d - 1],
            dst_ref=ring_ref.at[d - 1],
            send_sem=ring_send.at[d - 1],
            recv_sem=ring_recv.at[d - 1],
            device_id={"pts": lax.rem(me + d, owners)},
            device_id_type=MESH,
        )
        copy.start()
        rings.append(copy)
    loads[1].wait()
    for a in range(half):
        real = slip_ref[my_slip, 0:1, a * LANES : (a + 1) * LANES]
        imag = slip_ref[my_slip, 1:2, a * LANES : (a + 1) * LANES]
        spect_ref[a : a + 1, :] = real
        spect_ref[half + a : half + a + 1, :] = real
        spect_ref[2 * half + a : 2 * half + a + 1, :] = -imag
        spect_ref[3 * half + a : 3 * half + a + 1, :] = imag
    turned = jnp.transpose(spect_ref[...])
    for copy in loads[2:]:
        copy.wait()
    slip_real = weight_ref[...] * jnp.concatenate(
        [turned[:blocks, :blocks], turned[blocks:, :blocks]], axis=1
    )
    slip_imag = weight_ref[...] * jnp.concatenate(
        [turned[:blocks, blocks:], turned[blocks:, blocks:]], axis=1
    )
    spect_ref[:blocks, :] = slip_real
    spect_ref[blocks:, :] = slip_imag

    packed = joined(0)
    for copy in rings:
        copy.wait_recv()
    for d in range(1, owners):
        packed = packed + ring_ref[d - 1]

    stage = left(first_ref, packed)
    cos, sin = twiddle_ref[0], twiddle_ref[1]
    rows = []
    for c in range(comps):
        real = stage[2 * c * blocks : (2 * c + 1) * blocks]
        imag = stage[(2 * c + 1) * blocks : (2 * c + 2) * blocks]
        rows.append(
            jnp.concatenate([real * cos + imag * sin, imag * cos - real * sin], axis=1)
        )
    spectra = right(jnp.concatenate(rows, axis=0), second_ref)
    slip_real, slip_imag = spect_ref[:blocks, :], spect_ref[blocks:, :]
    rows = []
    for c in range(comps):
        part = spectra[c * blocks : (c + 1) * blocks]
        rows.append(part[:, :LANES] * slip_real + part[:, LANES:] * slip_imag)
    middle = right(jnp.concatenate(rows, axis=0), third_ref)
    columns = []
    for c in range(comps):
        real = middle[c * blocks : (c + 1) * blocks, :LANES]
        imag = middle[c * blocks : (c + 1) * blocks, LANES:]
        columns.append(
            jnp.concatenate([real * cos - imag * sin, real * sin + imag * cos], axis=0)
        )
    result = left(last_ref, jnp.concatenate(columns, axis=1))
    for c in range(comps):
        out_ref[c] = result[:, c * LANES : (c + 1) * LANES]
    for copy in pairs + rings:
        copy.wait_send()


def per_device(owners, variants, cores, *args):
    sgt, moment, slip_spec, rp_slab, rup_counts, var_rupture, var_source, owner_map = args
    moments, comps, slab_dev, samples = sgt.shape
    nrp = rp_slab.shape[0]
    half = samples // LANES
    nv = owners * cores
    assert owner_map.shape[0] == nv * variants and 4 * half == LANES and nv % 8 == 0
    assert moments + 2 <= 8 and rup_counts.shape[1] <= 8
    lanes_q = ceil_to(nrp, LANES)
    delays = MOST * owners
    tail_rows = ceil_to(TAU * (delays - 1), LANES) // LANES
    width = samples + tail_rows * LANES
    pitch = ceil_to(comps * (half + tail_rows), 8)
    consts = tables(comps, samples, tail_rows, pitch)
    dims = (owners, variants, cores, lanes_q, delays, pitch, tail_rows)
    f32 = jnp.float32
    others = max(owners - 1, 1)
    smem = pl.BlockSpec(memory_space=pltpu.SMEM)
    vmem = pl.BlockSpec(memory_space=pltpu.VMEM)
    anywhere = pl.BlockSpec(memory_space=pl.ANY)
    out = pl.pallas_call(
        functools.partial(kernel, dims),
        out_shape=pltpu.VMEM((comps, half, LANES), f32),
        in_specs=[smem] * 5 + [vmem] + [anywhere] * 8,
        out_specs=vmem,
        scratch_shapes=[
            pltpu.VMEM(sgt.shape, sgt.dtype),
            pltpu.VMEM(slip_spec.shape, f32),
            *[pltpu.VMEM(t.shape, t.dtype) for t in consts],
            pltpu.VMEM((owners, 24, lanes_q), f32),
            pltpu.VMEM((1, lanes_q), jnp.int32),
            pltpu.VMEM((LANES, LANES), f32),
            pltpu.VMEM((comps, nv, width) if nv * delays > 64 else (1, 8, LANES), f32),
            pltpu.VMEM((nv * pitch, LANES), f32),
            pltpu.VMEM((cores - 1, owners * pitch, LANES), f32),
            pltpu.VMEM((others, pitch, LANES), f32),
            pltpu.VMEM((others, pitch, LANES), f32),
            pltpu.SemaphoreType.DMA((8,)),
            pltpu.SemaphoreType.DMA((owners,)),
            pltpu.SemaphoreType.DMA((owners,)),
            pltpu.SemaphoreType.DMA((cores,)),
            pltpu.SemaphoreType.DMA((cores,)),
            pltpu.SemaphoreType.DMA((owners,)),
            pltpu.SemaphoreType.DMA((owners,)),
        ],
        compiler_params=pltpu.CompilerParams(collective_id=0, has_side_effects=True),
    )(
        rup_counts,
        moment,
        var_rupture,
        var_source.T,
        owner_map,
        rp_slab.reshape(1, nrp),
        sgt,
        slip_spec,
        *[jnp.asarray(t) for t in consts],
    )
    return out.reshape(1, comps, samples)


def solution(mesh):
    placed = (
        P("cmp", None, ("site", "pts"), None),
        P("cmp", ("site", "pts")),
        P(),
        P("site"),
        P(("site", "pts"), None),
        P("site"),
        P("site", None),
        P("site"),
    )
    sizes = (mesh.shape["pts"], mesh.shape["var"], mesh.shape["cmp"])
    return jax.shard_map(
        functools.partial(per_device, *sizes),
        mesh=mesh,
        in_specs=placed,
        out_specs=P(("site", "pts", "var", "cmp"), None, None),
        check_vma=False,
    )
```
